256 devices in a mesh: ga: 2 (over z), ta: 16 (over y, core), gy: 8 (over x).
Axes of the slice: x: 8, y: 8, z: 2, core: 2. Of those that a mesh axis runs over, the one named last changes fastest.
The devices are a block of a 8x8x16 slice.
Arguments:
- clip: bfloat16 [128, 32, 64, 512], P(('ga', 'ta'), 'gy'), parts along dimension 0, may hold values from -6 to 6
- w_space: bfloat16 [3, 3, 512, 512], replicated, may hold values from -0.09375 to 0.09375
- w_time: bfloat16 [3, 512, 512], replicated, may hold values from -0.15625 to 0.15625
- w_qkv: bfloat16 [512, 1536], replicated, may hold values from -0.61871843 to 0.61871843
- w_out: bfloat16 [512, 512], replicated, may hold values from -0.25 to 0.25
- norm_gain: float32 [512], replicated, may hold values from 0.1 to 1.9
Outputs:
- block_out: bfloat16 [128, 32, 64, 512], P(('ga', 'ta'), 'gy'), parts along dimension 0
The draws below stay inside these ranges and needn't reach their ends.
There are 2 independent parts, one for each index of `ga`. The reference program is written for one: setup_inputs(seed, part) draws one part's arguments, and reference() takes and returns one part's arrays. A program takes and returns all parts, laid end to end along the dimension named above; an argument that names none is the same for every part. Nothing has to cross between parts.
All inputs are finite; a program needn't handle non-finite values.
Results may differ from the reference program's by a relative error of at most 0.0085.
Values may be sent and summed in bfloat16 or wider, within the bound.
A program may use at most 64 MiB of HBM per device.

```python
import jax
import jax.numpy as jnp
from jax import lax

C = 512
HEADS = 8
WIDTH_CELLS = 64
FRAMES = 64
ROWS = 32


def draw_clip(key, part):
    full_shape = (FRAMES, ROWS, WIDTH_CELLS, C)
    normal_draw = jax.random.truncated_normal(jax.random.fold_in(key, 11), -6.0, 6.0, full_shape, jnp.float32)
    return normal_draw.astype(jnp.bfloat16)


def draw_w_qkv(key, part):
    head_width = C // HEADS
    full_shape = (C, 3, HEADS, head_width)
    weights = jax.random.truncated_normal(jax.random.fold_in(key, 23), -6.0, 6.0, full_shape, jnp.float32) * C ** (-0.5)
    return weights.reshape(C, 3 * C).astype(jnp.bfloat16)


def bell_draw(key, shape, scale, reach, kind=jnp.bfloat16):
    entries = scale * jax.random.normal(key, shape, jnp.float32)
    return jnp.clip(entries, min=-reach, max=reach).astype(kind)


def setup_inputs(seed: int = 0, part: int = 0) -> dict:
    seeds = jax.random.split(jax.random.key(seed), 7)
    part_keys = jax.random.split(jax.random.fold_in(seeds[6], part), 7)
    clip = draw_clip(jax.random.fold_in(jax.random.fold_in(seeds[6], part), 71), part)
    w_space = bell_draw(seeds[1], (3, 3, C, C), (9 * C) ** -0.5, 0.09375)
    w_time = bell_draw(seeds[2], (3, C, C), (3 * C) ** -0.5, 0.15625)
    w_qkv = draw_w_qkv(jax.random.fold_in(seeds[6], 71), part)
    w_out = bell_draw(seeds[4], (C, C), C ** -0.5, 0.25)
    norm_gain = jnp.clip(1.0 + 0.18 * jax.random.normal(seeds[5], (C,), jnp.float32), 0.1, 1.9)
    return {"clip": clip, "w_space": w_space, "w_time": w_time, "w_qkv": w_qkv, "w_out": w_out, "norm_gain": norm_gain}


def conv_space(padded, w_space, height, width):
    channels = padded.shape[-1]
    total = jnp.zeros(padded.shape[:1] + (height, width, channels), jnp.float32)
    for row_off in range(3):
        for col_off in range(3):
            window = padded[:, row_off:row_off + height, col_off:col_off + width, :]
            product = jnp.dot(window.reshape(-1, channels), w_space[row_off, col_off], preferred_element_type=jnp.float32)
            total = total + product.reshape(total.shape)
    return total

def temporal_mix(clip, hidden, earlier, w_time, norm_gain):
    channels = clip.shape[-1]
    frames = hidden.shape[0]
    joined = jnp.concatenate([earlier, hidden], axis=0)
    total = jnp.zeros(hidden.shape, jnp.float32)
    for tap_index in range(3):
        window = joined[2 - tap_index:2 - tap_index + frames]
        product = jnp.dot(window.reshape(-1, channels), w_time[tap_index], preferred_element_type=jnp.float32)
        total = total + product.reshape(hidden.shape)
    mixed = (clip.astype(jnp.float32) + total).astype(jnp.bfloat16)
    wide = mixed.astype(jnp.float32)
    scale = lax.rsqrt(lax.optimization_barrier(jnp.mean(wide * wide, axis=-1, keepdims=True)) + 1e-06)
    normed = (wide * scale * norm_gain).astype(jnp.bfloat16)
    return (mixed, normed)

def project(normed, w_qkv):
    channels = normed.shape[-1]
    flattened = jnp.dot(normed.reshape(-1, channels), w_qkv, preferred_element_type=jnp.float32).astype(jnp.bfloat16)
    joined = flattened.reshape(normed.shape[:-1] + (3 * channels,))
    return (joined[..., :channels], joined[..., channels:2 * channels], joined[..., 2 * channels:])

def attend(queries, keyset, valueset, heads):
    frames, rows, cols, channels = queries.shape
    head_dim = channels // heads
    shape = (frames, rows, cols, heads, head_dim)
    query_f = queries.reshape(shape).astype(jnp.float32)
    key_f = keyset.reshape(shape).astype(jnp.float32)
    value_f = valueset.reshape(shape).astype(jnp.float32)
    scores = jnp.einsum('frwhd,grwhd->rwhfg', query_f, key_f) * (1.0 / head_dim ** 0.5)
    peak = lax.optimization_barrier(jnp.max(scores, axis=-1, keepdims=True))
    expo = jnp.exp(scores - peak)
    probs = (expo / lax.optimization_barrier(jnp.sum(expo, axis=-1, keepdims=True))).astype(jnp.bfloat16)
    output = jnp.einsum('rwhfg,grwhd->frwhd', probs.astype(jnp.float32), value_f)
    return output.reshape(queries.shape).astype(jnp.bfloat16)

def reference(clip, w_space, w_time, w_qkv, w_out, norm_gain):
    frames, height, width, channels = clip.shape
    padded = jnp.pad(clip, ((0, 0), (1, 1), (1, 1), (0, 0)))
    hidden = jax.nn.silu(conv_space(padded, w_space, height, width)).astype(jnp.bfloat16)
    earlier = jnp.zeros((2,) + hidden.shape[1:], jnp.bfloat16)
    mixed, normed = temporal_mix(clip, hidden, earlier, w_time, norm_gain)
    queries, keyset, valueset = project(normed, w_qkv)

    def one_row(triple):
        return attend(triple[0], triple[1], triple[2], HEADS)
    stacked = tuple((jnp.moveaxis(item, 1, 0)[:, :, None] for item in (queries, keyset, valueset)))
    attended = lax.map(one_row, stacked)
    attended = jnp.moveaxis(attended[:, :, 0], 0, 1)
    projected = jnp.dot(attended.reshape(-1, channels), w_out, preferred_element_type=jnp.float32).reshape(clip.shape)
    return (mixed.astype(jnp.float32) + projected).astype(jnp.bfloat16)
```

```python
import functools

import jax
import jax.numpy as jnp
from jax import lax
from jax.experimental import pallas as pl
from jax.experimental.pallas import tpu as pltpu
from jax.sharding import PartitionSpec as P

HEADS = 8
MESH = pl.DeviceIdType.MESH
F32 = jnp.float32
BF16 = jnp.bfloat16


def dot(a, b):
    return jnp.dot(a, b, preferred_element_type=F32)


def dot_t(a, b):
    return lax.dot_general(a, b, (((1,), (1,)), ((), ())), preferred_element_type=F32)


def block_kernel(
    n,
    ny,
    clip,
    w_space,
    w_time,
    w_qkv,
    w_out,
    gain,
    out,
    xv,
    hv,
    mixed,
    sv,
    rv,
    av,
    ov,
    qkv,
    bias,
    perm,
    outv,
    ws,
    wt,
    wq,
    wo,
    gv,
    clip_sem,
    ws_sem,
    w_sem,
    x_send,
    x_recv,
    h_send,
    h_recv,
    a_send,
    a_recv,
    b_send,
    b_recv,
    o_sem,
):
    frames, rows, width, channels = clip.shape
    tokens = frames * width
    cols = width // n
    piece = frames * cols
    t = lax.axis_index("ta")
    g = lax.axis_index("gy")
    chips = n // 2
    chip, core = t // 2, lax.rem(t, 2)

    def peer(chip_off, core_off):
        return lax.rem(chip + chip_off + chips, chips) * 2 + lax.rem(core + core_off, 2)

    half = chips // 2
    offsets = [half]
    for d in range(half - 1, 0, -1):
        offsets += [d, -d]
    peers = [(c, k) for c in offsets for k in (0, 1)] + [(0, 1)]

    barrier = pltpu.get_barrier_semaphore()
    for c, k in peers:
        pl.semaphore_signal(barrier, inc=1, device_id={"ta": peer(c, k)}, device_id_type=MESH)

    @pl.when(g > 0)
    def _():
        pl.semaphore_signal(barrier, inc=1, device_id={"gy": g - 1}, device_id_type=MESH)

    @pl.when(g < ny - 1)
    def _():
        pl.semaphore_signal(barrier, inc=1, device_id={"gy": g + 1}, device_id_type=MESH)

    clip_loads = [
        pltpu.make_async_copy(clip.at[:, r], xv.at[r + 1], clip_sem.at[r]) for r in range(rows)
    ]
    for load in clip_loads:
        load.start()
    space_loads = []
    for b in range(3):
        for a in range(3):
            load = pltpu.make_async_copy(
                w_space.at[a, b], ws.at[b, pl.ds(a * channels, channels)], ws_sem.at[b, a]
            )
            load.start()
            space_loads.append(load)
    other_loads = [
        pltpu.make_async_copy(w_time, wt, w_sem.at[0]),
        pltpu.make_async_copy(w_qkv, wq, w_sem.at[1]),
        pltpu.make_async_copy(w_out, wo, w_sem.at[2]),
        pltpu.make_async_copy(gain, gv, w_sem.at[3]),
    ]
    for load in other_loads:
        load.start()

    row_i = lax.broadcasted_iota(jnp.int32, (tokens, tokens), 0)
    col_i = lax.broadcasted_iota(jnp.int32, (tokens, tokens), 1)
    same = lax.rem(row_i, cols) == lax.rem(col_i, cols)
    bias[...] = jnp.where(same, 0.0, -1e30)
    natural = (
        lax.rem(row_i // cols, frames) * width + (row_i // piece) * cols + lax.rem(row_i, cols)
    )
    perm[0] = jnp.where(natural == col_i, 1.0, 0.0).astype(BF16)
    natural_t = (
        lax.rem(col_i // cols, frames) * width + (col_i // piece) * cols + lax.rem(col_i, cols)
    )
    perm[1] = jnp.where(natural_t == row_i, 1.0, 0.0).astype(BF16)

    @pl.when(g == 0)
    def _():
        xv[0] = jnp.zeros(xv.shape[1:], BF16)

    @pl.when(g == ny - 1)
    def _():
        xv[rows + 1] = jnp.zeros(xv.shape[1:], BF16)

    @pl.when(t == 0)
    def _():
        hv[:, 0:2] = jnp.zeros((rows, 2) + hv.shape[2:], BF16)

    column = lax.rem(lax.broadcasted_iota(jnp.int32, (tokens, channels), 0), width)

    def conv_row(r):
        lhs = jnp.concatenate([xv[r + a].reshape(tokens, channels) for a in range(3)], axis=1)
        left = pltpu.roll(dot(lhs, ws[0]), 1, 0)
        total = jnp.where(column == 0, 0.0, left) + dot(lhs, ws[1])
        right = pltpu.roll(dot(lhs, ws[2]), tokens - 1, 0)
        total = total + jnp.where(column == width - 1, 0.0, right)
        hidden = (total * jax.nn.sigmoid(total)).astype(BF16)
        hv[r, 2:] = hidden.reshape(frames, width, channels)

    def hidden_copy(r):
        return pltpu.make_async_remote_copy(
            src_ref=hv.at[r, pl.ds(frames, 2)],
            dst_ref=hv.at[r, pl.ds(0, 2)],
            send_sem=h_send.at[r],
            recv_sem=h_recv.at[r],
            device_id={"ta": lax.rem(t + 1, n)},
            device_id_type=MESH,
        )

    def send_hidden(r):
        @pl.when(t < n - 1)
        def _():
            hidden_copy(r).start()

    def exchange(src, dst, r, dest, send_sem, recv_sem):
        return pltpu.make_async_remote_copy(
            src_ref=src.at[r, pl.ds(pl.multiple_of(dest * piece, piece), piece)],
            dst_ref=dst.at[r, pl.ds(pl.multiple_of(t * piece, piece), piece)],
            send_sem=send_sem.at[r],
            recv_sem=recv_sem.at[r],
            device_id={"ta": dest},
            device_id_type=MESH,
        )

    def send_all(src, dst, r, send_sem, recv_sem):
        for c, k in peers:
            exchange(src, dst, r, peer(c, k), send_sem, recv_sem).start()
        own = pl.ds(pl.multiple_of(t * piece, piece), piece)
        dst[r, own] = src[r, own]

    def whole(src, dst, r, send_sem, recv_sem):
        return pltpu.make_async_remote_copy(
            src_ref=src.at[r, pl.ds(0, (n - 1) * piece)],
            dst_ref=dst.at[r, pl.ds(0, (n - 1) * piece)],
            send_sem=send_sem.at[r],
            recv_sem=recv_sem.at[r],
            device_id={"ta": lax.rem(t + 1, n)},
            device_id_type=MESH,
        )

    def temporal_row(r):
        @pl.when(t > 0)
        def _():
            hidden_copy(r).wait_recv()

        lhs = jnp.concatenate(
            [hv[r, 2 - k : 2 - k + frames].reshape(tokens, channels) for k in range(3)], axis=1
        )
        total = xv[r + 1].reshape(tokens, channels).astype(F32) + dot(lhs, wt[...])
        rounded = total.astype(BF16)
        mixed[r] = rounded
        wide = rounded.astype(F32)
        scale = lax.rsqrt(jnp.mean(wide * wide, axis=-1, keepdims=True) + 1e-06)
        normed = (wide * scale * gv[...]).astype(BF16)
        sv[r] = dot(perm[0], normed).astype(BF16)
        send_all(sv, rv, r, a_send, a_recv)

    for load in clip_loads + space_loads:
        load.wait()
    lax.fori_loop(1, rows - 1, lambda r, c: (conv_row(r), c)[1], 0)
    for load in other_loads:
        load.wait()

    greeted = n - 1 + jnp.where(g > 0, 1, 0) + jnp.where(g < ny - 1, 1, 0)
    pl.semaphore_wait(barrier, greeted)

    up = pltpu.make_async_remote_copy(
        src_ref=xv.at[1],
        dst_ref=xv.at[rows + 1],
        send_sem=x_send.at[0],
        recv_sem=x_recv.at[0],
        device_id={"gy": lax.rem(g + ny - 1, ny)},
        device_id_type=MESH,
    )
    down = pltpu.make_async_remote_copy(
        src_ref=xv.at[rows],
        dst_ref=xv.at[0],
        send_sem=x_send.at[1],
        recv_sem=x_recv.at[1],
        device_id={"gy": lax.rem(g + 1, ny)},
        device_id_type=MESH,
    )

    @pl.when(g > 0)
    def _():
        up.start()

    @pl.when(g < ny - 1)
    def _():
        down.start()

    for r in range(1, rows - 1):
        send_hidden(r)
    lax.fori_loop(1, rows - 1, lambda r, c: (temporal_row(r), c)[1], 0)

    @pl.when(g > 0)
    def _():
        down.wait_recv()

    @pl.when(g < ny - 1)
    def _():
        up.wait_recv()

    def edge(i, c):
        r = i * (rows - 1)
        conv_row(r)
        send_hidden(r)
        return c

    lax.fori_loop(0, 2, edge, 0)
    lax.fori_loop(0, 2, lambda i, c: (temporal_row(i * (rows - 1)), c)[1], 0)

    lane = lax.broadcasted_iota(jnp.int32, (tokens, 128), 1)
    head_dim = channels // HEADS

    def order(i):
        return jnp.where(i < rows - 2, i + 1, (i - (rows - 2)) * (rows - 1))

    def attend_row(i, carry):
        r = order(i)
        whole(sv, rv, r, a_send, a_recv).wait_recv()
        qkv[...] = dot(rv[r], wq[...]).astype(BF16)

        def pair(p, c):
            base = pl.multiple_of(p * 128, 128)
            q = qkv[:, pl.ds(base, 128)]
            k = qkv[:, pl.ds(pl.multiple_of(channels + p * 128, 128), 128)]
            v = qkv[:, pl.ds(pl.multiple_of(2 * channels + p * 128, 128), 128)]
            results = []
            for h in range(2):
                mine = (lane >= head_dim) if h else (lane < head_dim)
                q_h = jnp.where(mine, q, jnp.zeros_like(q))
                scores = dot_t(q_h, k) * (1.0 / head_dim**0.5) + bias[...]
                peak = jnp.max(scores, axis=-1, keepdims=True)
                expo = jnp.exp(scores - peak)
                total = jnp.sum(expo, axis=-1, keepdims=True)
                probs = (expo * (1.0 / total)).astype(BF16)
                results.append(dot(probs, v))
            av[r, :, pl.ds(base, 128)] = jnp.where(
                lane < head_dim, results[0], results[1]
            ).astype(BF16)
            return c

        lax.fori_loop(0, channels // 128, pair, 0)
        send_all(av, ov, r, b_send, b_recv)
        return carry

    lax.fori_loop(0, rows, attend_row, 0)

    def store(r):
        return pltpu.make_async_copy(outv.at[r], out.at[:, r], o_sem.at[r])

    def out_row(i, carry):
        r = order(i)
        whole(av, ov, r, b_send, b_recv).wait_recv()
        attended = dot(perm[1], ov[r]).astype(BF16)
        total = mixed[r].astype(F32) + dot(attended, wo[...])
        outv[r] = total.astype(BF16).reshape(frames, width, channels)
        store(r).start()
        return carry

    lax.fori_loop(0, rows, out_row, 0)

    @pl.when(g > 0)
    def _():
        up.wait_send()

    @pl.when(g < ny - 1)
    def _():
        down.wait_send()

    for r in range(rows):

        @pl.when(t < n - 1)
        def _():
            hidden_copy(r).wait_send()

        whole(sv, rv, r, a_send, a_recv).wait_send()
        whole(av, ov, r, b_send, b_recv).wait_send()
        store(r).wait()


def solution(mesh):
    n, ny = mesh.shape["ta"], mesh.shape["gy"]

    def per_device(clip, w_space, w_time, w_qkv, w_out, norm_gain):
        frames, rows, width, channels = clip.shape
        tokens = frames * width
        row_tokens = (rows, tokens, channels)
        dma = pltpu.SemaphoreType.DMA
        return pl.pallas_call(
            functools.partial(block_kernel, n, ny),
            out_shape=jax.ShapeDtypeStruct(clip.shape, BF16),
            in_specs=[pl.BlockSpec(memory_space=pl.ANY)] * 6,
            out_specs=pl.BlockSpec(memory_space=pl.ANY),
            scratch_shapes=[
                pltpu.VMEM((rows + 2, frames, width, channels), BF16),
                pltpu.VMEM((rows, frames + 2, width, channels), BF16),
                pltpu.VMEM(row_tokens, BF16),
                pltpu.VMEM(row_tokens, BF16),
                pltpu.VMEM(row_tokens, BF16),
                pltpu.VMEM(row_tokens, BF16),
                pltpu.VMEM(row_tokens, BF16),
                pltpu.VMEM((tokens, 3 * channels), BF16),
                pltpu.VMEM((tokens, tokens), F32),
                pltpu.VMEM((2, tokens, tokens), BF16),
                pltpu.VMEM((rows, frames, width, channels), BF16),
                pltpu.VMEM((3, 3 * channels, channels), BF16),
                pltpu.VMEM((3 * channels, channels), BF16),
                pltpu.VMEM((channels, 3 * channels), BF16),
                pltpu.VMEM((channels, channels), BF16),
                pltpu.VMEM((1, channels), F32),
                dma((rows,)),
                dma((3, 3)),
                dma((4,)),
                dma((2,)),
                dma((2,)),
                dma((rows,)),
                dma((rows,)),
                dma((rows,)),
                dma((rows,)),
                dma((rows,)),
                dma((rows,)),
                dma((rows,)),
            ],
            compiler_params=pltpu.CompilerParams(
                collective_id=0, has_side_effects=True, vmem_limit_bytes=48 * 2**20
            ),
        )(
            clip,
            w_space,
            w_time.reshape(3 * channels, channels),
            w_qkv,
            w_out,
            norm_gain.reshape(1, channels),
        )

    in_specs = (P(("ga", "ta"), "gy", None, None), P(), P(), P(), P(), P())
    out_specs = P(("ga", "ta"), "gy", None, None)
    return jax.shard_map(
        per_device, mesh=mesh, in_specs=in_specs, out_specs=out_specs, check_vma=False
    )
```

```python
import functools

import jax
import jax.numpy as jnp
from jax import lax
from jax.experimental import pallas as pl
from jax.experimental.pallas import tpu as pltpu
from jax.sharding import PartitionSpec as P

HEADS = 8
MESH = pl.DeviceIdType.MESH
F32 = jnp.float32
BF16 = jnp.bfloat16


def dot(a, b):
    return jnp.dot(a, b, preferred_element_type=F32)


def dot_t(a, b):
    return lax.dot_general(a, b, (((1,), (1,)), ((), ())), preferred_element_type=F32)


def block_kernel(
    n,
    ny,
    clip,
    w_space,
    w_time,
    w_qkv,
    w_out,
    gain,
    out,
    xv,
    hv,
    mixed,
    sv,
    rv,
    av,
    ov,
    qkv,
    bias,
    perm,
    ws,
    wt,
    wq,
    wo,
    gv,
    clip_sem,
    ws_sem,
    w_sem,
    x_send,
    x_recv,
    h_send,
    h_recv,
    a_send,
    a_recv,
    b_send,
    b_recv,
    late,
    x_ready,
):
    frames, rows, width, channels = clip.shape
    tokens = frames * width
    cols = width // n
    piece = frames * cols
    t = lax.axis_index("ta")
    g = lax.axis_index("gy")
    chips = n // 2
    chip, core = t // 2, lax.rem(t, 2)

    def peer(chip_off, core_off):
        return lax.rem(chip + chip_off + chips, chips) * 2 + lax.rem(core + core_off, 2)

    half = chips // 2
    offsets = [half]
    for d in range(half - 1, 0, -1):
        offsets += [d, -d]
    peers = [(c, k) for c in offsets for k in (0, 1)] + [(0, 1)]

    barrier = pltpu.get_barrier_semaphore()

    @pl.when(g > 0)
    def _():
        pl.semaphore_signal(barrier, inc=1, device_id={"gy": g - 1}, device_id_type=MESH)

    @pl.when(t > 0)
    def _():
        for c, k in peers:
            pl.semaphore_signal(barrier, inc=1, device_id={"ta": peer(c, k)}, device_id_type=MESH)

    above = jnp.where(g < ny - 1, 1, 0)

    clip_loads = [
        pltpu.make_async_copy(clip.at[:, r], xv.at[r + 1], clip_sem.at[r]) for r in range(rows)
    ]
    for load in clip_loads:
        load.start()
    space_loads = []
    for b in range(3):
        for a in range(3):
            load = pltpu.make_async_copy(
                w_space.at[a, b], ws.at[b, pl.ds(a * channels, channels)], ws_sem.at[b, a]
            )
            load.start()
            space_loads.append(load)
    other_loads = [
        pltpu.make_async_copy(w_time, wt, w_sem.at[0]),
        pltpu.make_async_copy(w_qkv, wq, w_sem.at[1]),
        pltpu.make_async_copy(w_out, wo, w_sem.at[2]),
        pltpu.make_async_copy(gain, gv, w_sem.at[3]),
    ]
    for load in other_loads:
        load.start()

    @pl.when(t == 0)
    def _():
        pl.semaphore_wait(barrier, n - 1 + above)
        for k in range(1, n):
            pl.semaphore_signal(late, inc=1, device_id={"ta": k}, device_id_type=MESH)

    row_i = lax.broadcasted_iota(jnp.int32, (tokens, tokens), 0)
    col_i = lax.broadcasted_iota(jnp.int32, (tokens, tokens), 1)
    same = lax.rem(row_i, cols) == lax.rem(col_i, cols)
    bias[...] = jnp.where(same, 0.0, -1e30)
    natural = (
        lax.rem(row_i // cols, frames) * width + (row_i // piece) * cols + lax.rem(row_i, cols)
    )
    perm[0] = jnp.where(natural == col_i, 1.0, 0.0).astype(BF16)
    natural_t = (
        lax.rem(col_i // cols, frames) * width + (col_i // piece) * cols + lax.rem(col_i, cols)
    )
    perm[1] = jnp.where(natural_t == row_i, 1.0, 0.0).astype(BF16)

    @pl.when(g == 0)
    def _():
        xv[0] = jnp.zeros(xv.shape[1:], BF16)

    @pl.when(g == ny - 1)
    def _():
        xv[rows + 1] = jnp.zeros(xv.shape[1:], BF16)

    @pl.when(t == 0)
    def _():
        hv[:, 0:2] = jnp.zeros((rows, 2) + hv.shape[2:], BF16)

    column = lax.rem(lax.broadcasted_iota(jnp.int32, (tokens, channels), 0), width)

    def conv_row(r):
        lhs = jnp.concatenate([xv[r + a].reshape(tokens, channels) for a in range(3)], axis=1)
        left = pltpu.roll(dot(lhs, ws[0]), 1, 0)
        total = jnp.where(column == 0, 0.0, left) + dot(lhs, ws[1])
        right = pltpu.roll(dot(lhs, ws[2]), tokens - 1, 0)
        total = total + jnp.where(column == width - 1, 0.0, right)
        hidden = (total * jax.nn.sigmoid(total)).astype(BF16)
        hv[r, 2:] = hidden.reshape(frames, width, channels)

    def hidden_copy(r):
        return pltpu.make_async_remote_copy(
            src_ref=hv.at[r, pl.ds(frames, 2)],
            dst_ref=hv.at[r, pl.ds(0, 2)],
            send_sem=h_send.at[r],
            recv_sem=h_recv.at[r],
            device_id={"ta": lax.rem(t + 1, n)},
            device_id_type=MESH,
        )

    def send_hidden(r):
        @pl.when(t < n - 1)
        def _():
            hidden_copy(r).start()

    def exchange(src, dst, r, dest, send_sem, recv_sem):
        return pltpu.make_async_remote_copy(
            src_ref=src.at[r, pl.ds(pl.multiple_of(dest * piece, piece), piece)],
            dst_ref=dst.at[r, pl.ds(pl.multiple_of(t * piece, piece), piece)],
            send_sem=send_sem.at[r],
            recv_sem=recv_sem.at[r],
            device_id={"ta": dest},
            device_id_type=MESH,
        )

    def send_all(src, dst, r, send_sem, recv_sem, skip_first):
        for c, k in peers:
            dest = peer(c, k)
            if skip_first:

                @pl.when(dest > 0)
                def _():
                    exchange(src, dst, r, dest, send_sem, recv_sem).start()

            else:
                exchange(src, dst, r, dest, send_sem, recv_sem).start()
        own = pl.ds(pl.multiple_of(t * piece, piece), piece)
        dst[r, own] = src[r, own]

    def whole(src, dst, r, send_sem, recv_sem):
        return pltpu.make_async_remote_copy(
            src_ref=src.at[r, pl.ds(0, (n - 1) * piece)],
            dst_ref=dst.at[r, pl.ds(0, (n - 1) * piece)],
            send_sem=send_sem.at[r],
            recv_sem=recv_sem.at[r],
            device_id={"ta": lax.rem(t + 1, n)},
            device_id_type=MESH,
        )

    def temporal_row(r):
        @pl.when(t > 0)
        def _():
            hidden_copy(r).wait_recv()

        lhs = jnp.concatenate(
            [hv[r, 2 - k : 2 - k + frames].reshape(tokens, channels) for k in range(3)], axis=1
        )
        total = xv[r + 1].reshape(tokens, channels).astype(F32) + dot(lhs, wt[...])
        rounded = total.astype(BF16)
        mixed[r] = rounded
        wide = rounded.astype(F32)
        scale = lax.rsqrt(jnp.mean(wide * wide, axis=-1, keepdims=True) + 1e-06)
        normed = (wide * scale * gv[...]).astype(BF16)
        sv[r] = dot(perm[0], normed).astype(BF16)
        send_all(sv, rv, r, a_send, a_recv, True)

    for load in clip_loads + space_loads:
        load.wait()
    lax.fori_loop(1, rows - 1, lambda r, c: (conv_row(r), c)[1], 0)
    for load in other_loads:
        load.wait()

    @pl.when(t > 0)
    def _():
        pl.semaphore_wait(barrier, n - 2 + above)

    up = pltpu.make_async_remote_copy(
        src_ref=xv.at[1],
        dst_ref=xv.at[rows + 1],
        send_sem=x_send.at[0],
        recv_sem=x_recv.at[0],
        device_id={"gy": lax.rem(g + ny - 1, ny)},
        device_id_type=MESH,
    )
    down = pltpu.make_async_remote_copy(
        src_ref=xv.at[rows],
        dst_ref=xv.at[0],
        send_sem=x_send.at[1],
        recv_sem=x_recv.at[1],
        device_id={"gy": lax.rem(g + 1, ny)},
        device_id_type=MESH,
    )

    for r in range(1, rows - 1):
        send_hidden(r)

    @pl.when(g < ny - 1)
    def _():
        pl.semaphore_signal(x_ready, inc=1, device_id={"gy": g + 1}, device_id_type=MESH)
        down.start()

    @pl.when(g > 0)
    def _():
        pl.semaphore_wait(x_ready, 1)
        up.start()

    temporal_row(1)

    @pl.when(g > 0)
    def _():
        down.wait_recv()

    @pl.when(g < ny - 1)
    def _():
        up.wait_recv()

    def edge(i, c):
        r = i * (rows - 1)
        conv_row(r)
        send_hidden(r)
        return c

    lax.fori_loop(0, 2, edge, 0)

    def order(i):
        return jnp.where(i < rows - 2, i + 1, (i - (rows - 2)) * (rows - 1))

    lax.fori_loop(1, rows, lambda i, c: (temporal_row(order(i)), c)[1], 0)

    @pl.when(t > 0)
    def _():
        pl.semaphore_wait(late, 1)
        for r in list(range(1, rows - 1)) + [0, rows - 1]:
            exchange(sv, rv, r, 0, a_send, a_recv).start()

    lane = lax.broadcasted_iota(jnp.int32, (tokens, 128), 1)
    head_dim = channels // HEADS

    def attend_row(i, carry):
        r = order(i)
        whole(sv, rv, r, a_send, a_recv).wait_recv()
        qkv[...] = dot(rv[r], wq[...]).astype(BF16)

        def pair(p, c):
            base = pl.multiple_of(p * 128, 128)
            q = qkv[:, pl.ds(base, 128)]
            k = qkv[:, pl.ds(pl.multiple_of(channels + p * 128, 128), 128)]
            v = qkv[:, pl.ds(pl.multiple_of(2 * channels + p * 128, 128), 128)]
            results = []
            for h in range(2):
                mine = (lane >= head_dim) if h else (lane < head_dim)
                q_h = jnp.where(mine, q, jnp.zeros_like(q))
                scores = dot_t(q_h, k) * (1.0 / head_dim**0.5) + bias[...]
                peak = jnp.max(scores, axis=-1, keepdims=True)
                expo = jnp.exp(scores - peak)
                total = jnp.sum(expo, axis=-1, keepdims=True)
                probs = (expo * (1.0 / total)).astype(BF16)
                results.append(dot(probs, v))
            av[r, :, pl.ds(base, 128)] = jnp.where(
                lane < head_dim, results[0], results[1]
            ).astype(BF16)
            return c

        lax.fori_loop(0, channels // 128, pair, 0)
        send_all(av, ov, r, b_send, b_recv, False)
        return carry

    lax.fori_loop(0, rows, attend_row, 0)

    def out_row(i, carry):
        r = order(i)
        whole(av, ov, r, b_send, b_recv).wait_recv()
        attended = dot(perm[1], ov[r]).astype(BF16)
        total = mixed[r].astype(F32) + dot(attended, wo[...])
        out[:, r] = total.astype(BF16).reshape(frames, width, channels)
        return carry

    lax.fori_loop(0, rows, out_row, 0)

    @pl.when(g > 0)
    def _():
        up.wait_send()

    @pl.when(g < ny - 1)
    def _():
        down.wait_send()

    for r in range(rows):

        @pl.when(t < n - 1)
        def _():
            hidden_copy(r).wait_send()

        whole(sv, rv, r, a_send, a_recv).wait_send()
        whole(av, ov, r, b_send, b_recv).wait_send()


def solution(mesh):
    n, ny = mesh.shape["ta"], mesh.shape["gy"]

    def per_device(clip, w_space, w_time, w_qkv, w_out, norm_gain):
        frames, rows, width, channels = clip.shape
        tokens = frames * width
        row_tokens = (rows, tokens, channels)
        dma = pltpu.SemaphoreType.DMA
        return pl.pallas_call(
            functools.partial(block_kernel, n, ny),
            out_shape=pltpu.VMEM(clip.shape, BF16),
            in_specs=[pl.BlockSpec(memory_space=pltpu.HBM)] * 6,
            out_specs=pl.BlockSpec(memory_space=pltpu.VMEM),
            scratch_shapes=[
                pltpu.VMEM((rows + 2, frames, width, channels), BF16),
                pltpu.VMEM((rows, frames + 2, width, channels), BF16),
                pltpu.VMEM(row_tokens, BF16),
                pltpu.VMEM(row_tokens, BF16),
                pltpu.VMEM(row_tokens, BF16),
                pltpu.VMEM(row_tokens, BF16),
                pltpu.VMEM(row_tokens, BF16),
                pltpu.VMEM((tokens, 3 * channels), BF16),
                pltpu.VMEM((tokens, tokens), F32),
                pltpu.VMEM((2, tokens, tokens), BF16),
                pltpu.VMEM((3, 3 * channels, channels), BF16),
                pltpu.VMEM((3 * channels, channels), BF16),
                pltpu.VMEM((channels, 3 * channels), BF16),
                pltpu.VMEM((channels, channels), BF16),
                pltpu.VMEM((1, channels), F32),
                dma((rows,)),
                dma((3, 3)),
                dma((4,)),
                dma((2,)),
                dma((2,)),
                dma((rows,)),
                dma((rows,)),
                dma((rows,)),
                dma((rows,)),
                dma((rows,)),
                dma((rows,)),
                pltpu.SemaphoreType.REGULAR,
                pltpu.SemaphoreType.REGULAR,
            ],
            compiler_params=pltpu.CompilerParams(
                collective_id=0, has_side_effects=True, vmem_limit_bytes=48 * 2**20
            ),
        )(
            *(
                pltpu.with_memory_space_constraint(a, pltpu.HBM)
                for a in (
                    clip,
                    w_space,
                    w_time.reshape(3 * channels, channels),
                    w_qkv,
                    w_out,
                    norm_gain.reshape(1, channels),
                )
            )
        )

    in_specs = (P(("ga", "ta"), "gy", None, None), P(), P(), P(), P(), P())
    out_specs = P(("ga", "ta"), "gy", None, None)
    return jax.shard_map(
        per_device, mesh=mesh, in_specs=in_specs, out_specs=out_specs, check_vma=False
    )
```

```python
import functools

import jax
import jax.numpy as jnp
from jax import lax
from jax.experimental import pallas as pl
from jax.experimental.pallas import tpu as pltpu
from jax.sharding import PartitionSpec as P

HEADS = 8
MESH = pl.DeviceIdType.MESH
F32 = jnp.float32
BF16 = jnp.bfloat16


def dot(a, b):
    return jnp.dot(a, b, preferred_element_type=F32)


def dot_t(a, b):
    return lax.dot_general(a, b, (((1,), (1,)), ((), ())), preferred_element_type=F32)


def block_kernel(
    n,
    ny,
    clip,
    w_space,
    w_time,
    w_qkv,
    w_out,
    gain,
    out,
    xv,
    hv,
    mixed,
    sv,
    rv,
    av,
    ov,
    qkv,
    scores,
    expo,
    summed,
    ones,
    att,
    perm,
    ws,
    wt,
    wq,
    wo,
    gv,
    clip_sem,
    ws_sem,
    w_sem,
    x_send,
    x_recv,
    h_send,
    h_recv,
    a_send,
    a_recv,
    b_send,
    b_recv,
    late,
    ready,
    next_ready,
):
    frames, rows, width, channels = clip.shape
    tokens = frames * width
    cols = width // n
    piece = frames * cols
    t = lax.axis_index("ta")
    g = lax.axis_index("gy")
    chips = n // 2
    chip, core = t // 2, lax.rem(t, 2)

    def peer(chip_off, core_off):
        return lax.rem(chip + chip_off + chips, chips) * 2 + lax.rem(core + core_off, 2)

    half = chips // 2
    offsets = [half]
    for d in range(half - 1, 0, -1):
        offsets += [d, -d]
    peers = [(c, k) for c in offsets for k in (0, 1)] + [(0, 1)]

    barrier = pltpu.get_barrier_semaphore()

    @pl.when(g > 0)
    def _():
        pl.semaphore_signal(barrier, inc=1, device_id={"gy": g - 1}, device_id_type=MESH)

    @pl.when(g < ny - 1)
    def _():
        pl.semaphore_signal(barrier, inc=1, device_id={"gy": g + 1}, device_id_type=MESH)

    @pl.when(t > 0)
    def _():
        for k in range(n):

            @pl.when((k > t) | (k == 0))
            def _():
                pl.semaphore_signal(barrier, inc=1, device_id={"ta": k}, device_id_type=MESH)

    beside = jnp.where(g < ny - 1, 1, 0) + jnp.where(g > 0, 1, 0)

    clip_loads = [
        pltpu.make_async_copy(clip.at[:, r], xv.at[r + 1], clip_sem.at[r]) for r in range(rows)
    ]
    for load in clip_loads:
        load.start()
    space_loads = []
    for b in range(3):
        for a in range(3):
            load = pltpu.make_async_copy(
                w_space.at[a, b], ws.at[b, pl.ds(a * channels, channels)], ws_sem.at[b, a]
            )
            load.start()
            space_loads.append(load)
    other_loads = [
        pltpu.make_async_copy(w_time, wt, w_sem.at[0]),
        pltpu.make_async_copy(w_qkv, wq, w_sem.at[1]),
        pltpu.make_async_copy(w_out, wo, w_sem.at[2]),
        pltpu.make_async_copy(gain, gv, w_sem.at[3]),
    ]

    row_i = lax.broadcasted_iota(jnp.int32, (tokens, tokens), 0)
    col_i = lax.broadcasted_iota(jnp.int32, (tokens, tokens), 1)
    clip_len = n * frames
    natural = (
        lax.rem(row_i // cols, frames) * width + (row_i // piece) * cols + lax.rem(row_i, cols)
    )
    perm[0] = jnp.where(natural == col_i, 1.0, 0.0).astype(BF16)
    natural_t = (
        lax.rem(col_i // cols, frames) * width + (col_i // piece) * cols + lax.rem(col_i, cols)
    )
    perm[1] = jnp.where(natural_t == row_i, 1.0, 0.0).astype(BF16)
    by_col = lax.rem(row_i, clip_len) * cols + row_i // clip_len
    perm[2] = jnp.where(by_col == col_i, 1.0, 0.0).astype(BF16)
    by_col_t = lax.rem(col_i, clip_len) * cols + col_i // clip_len
    perm[3] = jnp.where(by_col_t == row_i, 1.0, 0.0).astype(BF16)

    @pl.when(g == 0)
    def _():
        xv[0] = jnp.zeros(xv.shape[1:], BF16)

    @pl.when(g == ny - 1)
    def _():
        xv[rows + 1] = jnp.zeros(xv.shape[1:], BF16)

    @pl.when(t == 0)
    def _():
        hv[:, 0:2] = jnp.zeros((rows, 2) + hv.shape[2:], BF16)

    column = lax.rem(lax.broadcasted_iota(jnp.int32, (tokens, channels), 0), width)

    def conv_row(r):
        lhs = jnp.concatenate([xv[r + a].reshape(tokens, channels) for a in range(3)], axis=1)
        left = pltpu.roll(dot(lhs, ws[0]), 1, 0)
        total = jnp.where(column == 0, 0.0, left) + dot(lhs, ws[1])
        right = pltpu.roll(dot(lhs, ws[2]), tokens - 1, 0)
        total = total + jnp.where(column == width - 1, 0.0, right)
        hidden = (total * jax.nn.sigmoid(total)).astype(BF16)
        hv[r, 2:] = hidden.reshape(frames, width, channels)

    def hidden_copy(r):
        return pltpu.make_async_remote_copy(
            src_ref=hv.at[r, pl.ds(frames, 2)],
            dst_ref=hv.at[r, pl.ds(0, 2)],
            send_sem=h_send.at[r],
            recv_sem=h_recv.at[r],
            device_id={"ta": lax.rem(t + 1, n)},
            device_id_type=MESH,
        )

    def send_hidden(r):
        @pl.when(t < n - 1)
        def _():
            hidden_copy(r).start()

    def exchange(src, dst, r, dest, send_sem, recv_sem):
        return pltpu.make_async_remote_copy(
            src_ref=src.at[r, pl.ds(pl.multiple_of(dest * piece, piece), piece)],
            dst_ref=dst.at[r, pl.ds(pl.multiple_of(t * piece, piece), piece)],
            send_sem=send_sem.at[r],
            recv_sem=recv_sem.at[r],
            device_id={"ta": dest},
            device_id_type=MESH,
        )

    def send_all(src, dst, r, send_sem, recv_sem, skip_first):
        for c, k in peers:
            dest = peer(c, k)
            if skip_first:

                @pl.when(dest > 0)
                def _():
                    exchange(src, dst, r, dest, send_sem, recv_sem).start()

            else:
                exchange(src, dst, r, dest, send_sem, recv_sem).start()
        own = pl.ds(pl.multiple_of(t * piece, piece), piece)
        dst[r, own] = src[r, own]

    def whole(src, dst, r, send_sem, recv_sem):
        return pltpu.make_async_remote_copy(
            src_ref=src.at[r, pl.ds(0, (n - 1) * piece)],
            dst_ref=dst.at[r, pl.ds(0, (n - 1) * piece)],
            send_sem=send_sem.at[r],
            recv_sem=recv_sem.at[r],
            device_id={"ta": lax.rem(t + 1, n)},
            device_id_type=MESH,
        )

    def temporal_row(r):
        @pl.when(t > 0)
        def _():
            hidden_copy(r).wait_recv()

        lhs = jnp.concatenate(
            [hv[r, 2 - k : 2 - k + frames].reshape(tokens, channels) for k in range(3)], axis=1
        )
        total = xv[r + 1].reshape(tokens, channels).astype(F32) + dot(lhs, wt[...])
        rounded = total.astype(BF16)
        mixed[r] = rounded
        wide = rounded.astype(F32)
        scale = lax.rsqrt(jnp.mean(wide * wide, axis=-1, keepdims=True) + 1e-06)
        normed = (wide * scale * gv[...]).astype(BF16)
        sv[r] = dot(perm[0], normed).astype(BF16)

    up = pltpu.make_async_remote_copy(
        src_ref=clip.at[:, 0],
        dst_ref=xv.at[rows + 1],
        send_sem=x_send.at[0],
        recv_sem=x_recv.at[0],
        device_id={"gy": lax.rem(g + ny - 1, ny)},
        device_id_type=MESH,
    )
    down = pltpu.make_async_remote_copy(
        src_ref=clip.at[:, rows - 1],
        dst_ref=xv.at[0],
        send_sem=x_send.at[1],
        recv_sem=x_recv.at[1],
        device_id={"gy": lax.rem(g + 1, ny)},
        device_id_type=MESH,
    )
    pl.semaphore_wait(barrier, jnp.where(t == 0, n - 1, t - 1) + beside)

    @pl.when(g < ny - 1)
    def _():
        down.start()

    @pl.when(g > 0)
    def _():
        up.start()

    @pl.when(t > 1)
    def _():
        pl.semaphore_signal(next_ready, inc=1, device_id={"ta": t - 1}, device_id_type=MESH)

    for k in range(1, n):

        @pl.when(k < t)
        def _():
            pl.semaphore_signal(ready, inc=1, device_id={"ta": k}, device_id_type=MESH)

        @pl.when(t == 0)
        def _():
            pl.semaphore_signal(late, inc=1, device_id={"ta": k}, device_id_type=MESH)

    for load in clip_loads + space_loads:
        load.wait()
    for load in other_loads:
        load.start()
    lax.fori_loop(1, rows - 1, lambda r, c: (conv_row(r), c)[1], 0)

    @pl.when((t > 0) & (t < n - 1))
    def _():
        pl.semaphore_wait(next_ready, 1)

    for r in range(1, rows - 1):
        send_hidden(r)

    for load in other_loads:
        load.wait()

    def order(i):
        return jnp.where(i < rows - 2, i + 1, (i - (rows - 2)) * (rows - 1))

    def temporal(i, c):
        r = order(i)
        temporal_row(r)

        @pl.when((i == 0) & (t > 0) & (t < n - 1))
        def _():
            pl.semaphore_wait(ready, n - 1 - t)

        send_all(sv, rv, r, a_send, a_recv, True)
        return c

    before = jnp.where((t == 0) | (t >= n // 2), 1, 0)
    lax.fori_loop(0, before, temporal, 0)

    @pl.when(g > 0)
    def _():
        down.wait_recv()

    @pl.when(g < ny - 1)
    def _():
        up.wait_recv()

    def edge(i, c):
        r = i * (rows - 1)
        conv_row(r)
        send_hidden(r)
        return c

    lax.fori_loop(0, 2, edge, 0)
    lax.fori_loop(before, rows, temporal, 0)

    @pl.when(t > 0)
    def _():
        pl.semaphore_wait(late, 1)
        for r in list(range(1, rows - 1)) + [0, rows - 1]:
            exchange(sv, rv, r, 0, a_send, a_recv).start()

    head_dim = channels // HEADS
    quad = 4 * head_dim
    low = lax.broadcasted_iota(jnp.int32, (clip_len, 2 * head_dim), 1) < head_dim
    head_of = lax.broadcasted_iota(jnp.int32, (clip_len, quad), 1) // head_dim
    ones_row = lax.broadcasted_iota(jnp.int32, (4 * clip_len, quad), 0) // clip_len
    ones_col = lax.broadcasted_iota(jnp.int32, (4 * clip_len, quad), 1) // head_dim
    ones[...] = jnp.where(ones_row == ones_col, 1.0, 0.0).astype(BF16)
    log2e_scale = 1.4426950408889634 / head_dim**0.5
    columns = [slice(c * clip_len, (c + 1) * clip_len) for c in range(cols)]
    quads = [slice(base, base + quad) for base in range(0, channels, quad)]

    def split_heads(x):
        zero = jnp.zeros_like(x)
        return jnp.concatenate([jnp.where(head_of == h, x, zero) for h in range(4)], axis=0)

    def attend_row(i, carry):
        r = order(i)
        whole(sv, rv, r, a_send, a_recv).wait_recv()
        arrived = dot(perm[2], rv[r]).astype(BF16)
        qkv[...] = dot(arrived, wq[...]).astype(BF16)
        for here in columns:
            for four in quads:
                k = qkv[here, channels + four.start : channels + four.stop]
                scores[here, four] = dot_t(qkv[here, four], split_heads(k))
        for here in columns:
            for base in range(0, channels, 2 * head_dim):
                pair = slice(base, base + 2 * head_dim)
                s = scores[here, pair]
                peak_low = jnp.max(jnp.where(low, s, -jnp.inf), axis=-1, keepdims=True)
                peak_high = jnp.max(jnp.where(low, -jnp.inf, s), axis=-1, keepdims=True)
                peak = jnp.where(low, peak_low, peak_high)
                expo[here, pair] = jnp.exp2((s - peak) * log2e_scale).astype(BF16)
        for four in quads:
            for here in columns:
                v = qkv[here, 2 * channels + four.start : 2 * channels + four.stop]
                summed[here, four] = dot(expo[here, four], split_heads(v))
            total = dot(expo[:, four], ones[...])
            att[:, four] = (summed[:, four] / total).astype(BF16)
        av[r] = dot(perm[3], att[...]).astype(BF16)
        send_all(av, ov, r, b_send, b_recv, False)
        return carry

    lax.fori_loop(0, rows, attend_row, 0)

    def out_row(i, carry):
        r = order(i)
        whole(av, ov, r, b_send, b_recv).wait_recv()
        attended = dot(perm[1], ov[r]).astype(BF16)
        total = mixed[r].astype(F32) + dot(attended, wo[...])
        out[:, r] = total.astype(BF16).reshape(frames, width, channels)
        return carry

    lax.fori_loop(0, rows, out_row, 0)

    @pl.when(g > 0)
    def _():
        up.wait_send()

    @pl.when(g < ny - 1)
    def _():
        down.wait_send()

    for r in range(rows):

        @pl.when(t < n - 1)
        def _():
            hidden_copy(r).wait_send()

        whole(sv, rv, r, a_send, a_recv).wait_send()
        whole(av, ov, r, b_send, b_recv).wait_send()


def solution(mesh):
    n, ny = mesh.shape["ta"], mesh.shape["gy"]

    def per_device(clip, w_space, w_time, w_qkv, w_out, norm_gain):
        frames, rows, width, channels = clip.shape
        tokens = frames * width
        row_tokens = (rows, tokens, channels)
        dma = pltpu.SemaphoreType.DMA
        return pl.pallas_call(
            functools.partial(block_kernel, n, ny),
            out_shape=pltpu.VMEM(clip.shape, BF16),
            in_specs=[pl.BlockSpec(memory_space=pltpu.HBM)] * 6,
            out_specs=pl.BlockSpec(memory_space=pltpu.VMEM),
            scratch_shapes=[
                pltpu.VMEM((rows + 2, frames, width, channels), BF16),
                pltpu.VMEM((rows, frames + 2, width, channels), BF16),
                pltpu.VMEM(row_tokens, BF16),
                pltpu.VMEM(row_tokens, BF16),
                pltpu.VMEM(row_tokens, BF16),
                pltpu.VMEM(row_tokens, BF16),
                pltpu.VMEM(row_tokens, BF16),
                pltpu.VMEM((tokens, 3 * channels), BF16),
                pltpu.VMEM((tokens, channels), F32),
                pltpu.VMEM((tokens, channels), BF16),
                pltpu.VMEM((tokens, channels), F32),
                pltpu.VMEM((4 * n * frames, 4 * (channels // HEADS)), BF16),
                pltpu.VMEM((tokens, channels), BF16),
                pltpu.VMEM((4, tokens, tokens), BF16),
                pltpu.VMEM((3, 3 * channels, channels), BF16),
                pltpu.VMEM((3 * channels, channels), BF16),
                pltpu.VMEM((channels, 3 * channels), BF16),
                pltpu.VMEM((channels, channels), BF16),
                pltpu.VMEM((1, channels), F32),
                dma((rows,)),
                dma((3, 3)),
                dma((4,)),
                dma((2,)),
                dma((2,)),
                dma((rows,)),
                dma((rows,)),
                dma((rows,)),
                dma((rows,)),
                dma((rows,)),
                dma((rows,)),
                pltpu.SemaphoreType.REGULAR,
                pltpu.SemaphoreType.REGULAR,
                pltpu.SemaphoreType.REGULAR,
            ],
            compiler_params=pltpu.CompilerParams(
                collective_id=0, has_side_effects=True, vmem_limit_bytes=48 * 2**20
            ),
        )(
            *(
                pltpu.with_memory_space_constraint(a, pltpu.HBM)
                for a in (
                    clip,
                    w_space,
                    w_time.reshape(3 * channels, channels),
                    w_qkv,
                    w_out,
                    norm_gain.reshape(1, channels),
                )
            )
        )

    in_specs = (P(("ga", "ta"), "gy", None, None), P(), P(), P(), P(), P())
    out_specs = P(("ga", "ta"), "gy", None, None)
    return jax.shard_map(
        per_device, mesh=mesh, in_specs=in_specs, out_specs=out_specs, check_vma=False
    )
```

```python
import functools

import jax
import jax.numpy as jnp
from jax import lax
from jax.experimental import pallas as pl
from jax.experimental.pallas import tpu as pltpu
from jax.sharding import PartitionSpec as P

HEADS = 8
MESH = pl.DeviceIdType.MESH
F32 = jnp.float32
BF16 = jnp.bfloat16


def dot(a, b):
    return jnp.dot(a, b, preferred_element_type=F32)


def dot_t(a, b):
    return lax.dot_general(a, b, (((1,), (1,)), ((), ())), preferred_element_type=F32)


def block_kernel(
    n,
    ny,
    clip,
    w_space,
    w_time,
    w_qkv,
    w_out,
    gain,
    out,
    xv,
    hv,
    mixed,
    sv,
    rv,
    av,
    ov,
    qkv,
    scores,
    expo,
    summed,
    ones,
    att,
    perm,
    ws,
    wt,
    wq,
    wo,
    gv,
    clip_sem,
    ws_sem,
    w_sem,
    x_send,
    x_recv,
    h_send,
    h_recv,
    a_send,
    a_recv,
    b_send,
    b_recv,
    late,
    ready,
    next_ready,
    passing,
    pass_send,
    pass_recv,
):
    frames, rows, width, channels = clip.shape
    tokens = frames * width
    cols = width // n
    piece = frames * cols
    t = lax.axis_index("ta")
    g = lax.axis_index("gy")
    chips = n // 2
    chip, core = t // 2, lax.rem(t, 2)

    def peer(chip_off, core_off):
        return lax.rem(chip + chip_off + chips, chips) * 2 + lax.rem(core + core_off, 2)

    half = chips // 2
    early = 2 * (chips - 1 - half)
    offsets = [half]
    for d in range(half - 1, 0, -1):
        offsets += [d, -d]
    peers = [(c, k) for c in offsets for k in (0, 1)] + [(0, 1)]

    barrier = pltpu.get_barrier_semaphore()

    @pl.when(g > 0)
    def _():
        pl.semaphore_signal(barrier, inc=1, device_id={"gy": g - 1}, device_id_type=MESH)

    @pl.when(g < ny - 1)
    def _():
        pl.semaphore_signal(barrier, inc=1, device_id={"gy": g + 1}, device_id_type=MESH)

    @pl.when(t > 0)
    def _():
        for k in range(n):

            @pl.when((k > t) | (k == 0))
            def _():
                pl.semaphore_signal(barrier, inc=1, device_id={"ta": k}, device_id_type=MESH)

    beside = jnp.where(g < ny - 1, 1, 0) + jnp.where(g > 0, 1, 0)

    clip_loads = [
        pltpu.make_async_copy(clip.at[:, r], xv.at[r + 1], clip_sem.at[r]) for r in range(rows)
    ]
    for load in clip_loads:
        load.start()
    space_loads = []
    for b in range(3):
        for a in range(3):
            load = pltpu.make_async_copy(
                w_space.at[a, b], ws.at[b, pl.ds(a * channels, channels)], ws_sem.at[b, a]
            )
            load.start()
            space_loads.append(load)
    other_loads = [
        pltpu.make_async_copy(w_time, wt, w_sem.at[0]),
        pltpu.make_async_copy(w_qkv, wq, w_sem.at[1]),
        pltpu.make_async_copy(w_out, wo, w_sem.at[2]),
        pltpu.make_async_copy(gain, gv, w_sem.at[3]),
    ]

    up = pltpu.make_async_remote_copy(
        src_ref=clip.at[:, 0],
        dst_ref=xv.at[rows + 1],
        send_sem=x_send.at[0],
        recv_sem=x_recv.at[0],
        device_id={"gy": lax.rem(g + ny - 1, ny)},
        device_id_type=MESH,
    )
    down = pltpu.make_async_remote_copy(
        src_ref=clip.at[:, rows - 1],
        dst_ref=xv.at[0],
        send_sem=x_send.at[1],
        recv_sem=x_recv.at[1],
        device_id={"gy": lax.rem(g + 1, ny)},
        device_id_type=MESH,
    )
    pl.semaphore_wait(barrier, jnp.where(t == 0, n - 1, t - 1) + beside)

    @pl.when(g < ny - 1)
    def _():
        down.start()

    @pl.when(g > 0)
    def _():
        up.start()

    @pl.when(t > 1)
    def _():
        pl.semaphore_signal(next_ready, inc=1, device_id={"ta": t - 1}, device_id_type=MESH)

    for k in range(1, n):

        @pl.when(k < t)
        def _():
            pl.semaphore_signal(ready, inc=1, device_id={"ta": k}, device_id_type=MESH)

        @pl.when(t == 0)
        def _():
            pl.semaphore_signal(late, inc=1, device_id={"ta": k}, device_id_type=MESH)

    row_i = lax.broadcasted_iota(jnp.int32, (tokens, tokens), 0)
    col_i = lax.broadcasted_iota(jnp.int32, (tokens, tokens), 1)
    clip_len = n * frames
    natural = (
        lax.rem(row_i // cols, frames) * width + (row_i // piece) * cols + lax.rem(row_i, cols)
    )
    perm[0] = jnp.where(natural == col_i, 1.0, 0.0).astype(BF16)
    natural_t = (
        lax.rem(col_i // cols, frames) * width + (col_i // piece) * cols + lax.rem(col_i, cols)
    )
    perm[1] = jnp.where(natural_t == row_i, 1.0, 0.0).astype(BF16)
    by_col = lax.rem(row_i, clip_len) * cols + row_i // clip_len
    perm[2] = jnp.where(by_col == col_i, 1.0, 0.0).astype(BF16)
    by_col_t = lax.rem(col_i, clip_len) * cols + col_i // clip_len
    perm[3] = jnp.where(by_col_t == row_i, 1.0, 0.0).astype(BF16)

    @pl.when(g == 0)
    def _():
        xv[0] = jnp.zeros(xv.shape[1:], BF16)

    @pl.when(g == ny - 1)
    def _():
        xv[rows + 1] = jnp.zeros(xv.shape[1:], BF16)

    @pl.when(t == 0)
    def _():
        hv[:, 0:2] = jnp.zeros((rows, 2) + hv.shape[2:], BF16)

    def conv_frames(r, first, count, arrived=lambda b: None):
        these = count * width
        column = lax.rem(lax.broadcasted_iota(jnp.int32, (these, channels), 0), width)
        here = pl.ds(first, count)
        lhs = jnp.concatenate(
            [xv[r + a, here].reshape(these, channels) for a in range(3)], axis=1
        )
        arrived(0)
        left = pltpu.roll(dot(lhs, ws[0]), 1, 0)
        arrived(1)
        total = jnp.where(column == 0, 0.0, left) + dot(lhs, ws[1])
        arrived(2)
        right = pltpu.roll(dot(lhs, ws[2]), these - 1, 0)
        total = total + jnp.where(column == width - 1, 0.0, right)
        hidden = (total * jax.nn.sigmoid(total)).astype(BF16)
        hv[r, pl.ds(first + 2, count)] = hidden.reshape(count, width, channels)

    def hidden_copy(r):
        return pltpu.make_async_remote_copy(
            src_ref=hv.at[r, pl.ds(frames, 2)],
            dst_ref=hv.at[r, pl.ds(0, 2)],
            send_sem=h_send.at[r],
            recv_sem=h_recv.at[r],
            device_id={"ta": lax.rem(t + 1, n)},
            device_id_type=MESH,
        )

    def send_hidden(r):
        @pl.when(t < n - 1)
        def _():
            hidden_copy(r).start()

    def exchange(src, dst, r, dest, send_sem, recv_sem):
        return pltpu.make_async_remote_copy(
            src_ref=src.at[r, pl.ds(pl.multiple_of(dest * piece, piece), piece)],
            dst_ref=dst.at[r, pl.ds(pl.multiple_of(t * piece, piece), piece)],
            send_sem=send_sem.at[r],
            recv_sem=recv_sem.at[r],
            device_id={"ta": dest},
            device_id_type=MESH,
        )

    def keep_own(src, dst, r):
        own = pl.ds(pl.multiple_of(t * piece, piece), piece)
        dst[r, own] = src[r, own]

    def send_normed(r, i):
        for c, k in peers:
            dest = peer(c, k)

            @pl.when((dest > 0) | (i > 0))
            def _():
                exchange(sv, rv, r, dest, a_send, a_recv).start()

        keep_own(sv, rv, r)

    step = half // 2

    def to_relay(k):
        dest = peer(half, k)
        return pltpu.make_async_remote_copy(
            src_ref=av.at[1, pl.ds(pl.multiple_of(dest * piece, piece), piece)],
            dst_ref=passing.at[pl.ds(k * piece, piece)],
            send_sem=b_send.at[1],
            recv_sem=pass_recv,
            device_id={"ta": peer(-step, 0)},
            device_id_type=MESH,
        )

    def from_relay(k):
        origin = peer(step, 0)
        return pltpu.make_async_remote_copy(
            src_ref=passing.at[pl.ds(k * piece, piece)],
            dst_ref=ov.at[1, pl.ds(pl.multiple_of(origin * piece, piece), piece)],
            send_sem=pass_send,
            recv_sem=b_recv.at[1],
            device_id={"ta": peer(-step, k)},
            device_id_type=MESH,
        )

    def pass_whole():
        return pltpu.make_async_remote_copy(
            src_ref=passing,
            dst_ref=passing,
            send_sem=pass_send,
            recv_sem=pass_recv,
            device_id={"ta": peer(-step, 0)},
            device_id_type=MESH,
        )

    def send_attended(r, i):
        for c, k in peers:
            if c == half:

                @pl.when(i == 0)
                def _():
                    to_relay(k).start()

                @pl.when(i > 0)
                def _():
                    exchange(av, ov, r, peer(c, k), b_send, b_recv).start()

            else:
                exchange(av, ov, r, peer(c, k), b_send, b_recv).start()
        keep_own(av, ov, r)

    def whole(src, dst, r, send_sem, recv_sem):
        return pltpu.make_async_remote_copy(
            src_ref=src.at[r, pl.ds(0, (n - 1) * piece)],
            dst_ref=dst.at[r, pl.ds(0, (n - 1) * piece)],
            send_sem=send_sem.at[r],
            recv_sem=recv_sem.at[r],
            device_id={"ta": lax.rem(t + 1, n)},
            device_id_type=MESH,
        )

    def temporal_row(r):
        @pl.when(t > 0)
        def _():
            hidden_copy(r).wait_recv()

        lhs = jnp.concatenate(
            [hv[r, 2 - k : 2 - k + frames].reshape(tokens, channels) for k in range(3)], axis=1
        )
        total = xv[r + 1].reshape(tokens, channels).astype(F32) + dot(lhs, wt[...])
        rounded = total.astype(BF16)
        mixed[r] = rounded
        wide = rounded.astype(F32)
        scale = lax.rsqrt(jnp.mean(wide * wide, axis=-1, keepdims=True) + 1e-06)
        normed = (wide * scale * gv[...]).astype(BF16)
        sv[r] = dot(perm[0], normed).astype(BF16)

    def space_arrived(b):
        for load in space_loads[3 * b : 3 * b + 3]:
            load.wait()

    for load in clip_loads:
        load.wait()
    conv_frames(1, frames - 2, 2, space_arrived)
    for load in other_loads:
        load.start()

    @pl.when((t > 0) & (t < n - 1))
    def _():
        pl.semaphore_wait(next_ready, 1)

    send_hidden(1)

    def inner_last(r, c):
        conv_frames(r, frames - 2, 2)
        send_hidden(r)
        return c

    def inner_first(r, c):
        conv_frames(r, 0, frames - 2)
        return c

    lax.fori_loop(2, rows - 1, inner_last, 0)
    lax.fori_loop(1, rows - 1, inner_first, 0)
    for load in other_loads:
        load.wait()

    def order(i):
        return jnp.where(i < rows - 2, i + 1, (i - (rows - 2)) * (rows - 1))

    def temporal(i, c):
        r = order(i)
        temporal_row(r)

        @pl.when((i == 0) & (t > 0) & (t < n - 1))
        def _():
            pl.semaphore_wait(ready, n - 1 - t)

        @pl.when((i == 1) & (t > 0))
        def _():
            pl.semaphore_wait(late, 1)
            exchange(sv, rv, order(0), 0, a_send, a_recv).start()

        send_normed(r, i)
        return c

    before = jnp.where((t == 0) | (t >= early), 1, 0)
    lax.fori_loop(0, before, temporal, 0)

    @pl.when(g > 0)
    def _():
        down.wait_recv()

    @pl.when(g < ny - 1)
    def _():
        up.wait_recv()

    def edge(i, c):
        r = i * (rows - 1)
        conv_frames(r, 0, frames)
        send_hidden(r)
        return c

    lax.fori_loop(0, 2, edge, 0)
    lax.fori_loop(before, rows, temporal, 0)

    head_dim = channels // HEADS
    quad = 4 * head_dim
    low = lax.broadcasted_iota(jnp.int32, (clip_len, 2 * head_dim), 1) < head_dim
    head_of = lax.broadcasted_iota(jnp.int32, (clip_len, quad), 1) // head_dim
    ones_row = lax.broadcasted_iota(jnp.int32, (4 * clip_len, quad), 0) // clip_len
    ones_col = lax.broadcasted_iota(jnp.int32, (4 * clip_len, quad), 1) // head_dim
    ones[...] = jnp.where(ones_row == ones_col, 1.0, 0.0).astype(BF16)
    log2e_scale = 1.4426950408889634 / head_dim**0.5
    columns = [slice(c * clip_len, (c + 1) * clip_len) for c in range(cols)]
    quads = [slice(base, base + quad) for base in range(0, channels, quad)]

    def split_heads(x):
        zero = jnp.zeros_like(x)
        return jnp.concatenate([jnp.where(head_of == h, x, zero) for h in range(4)], axis=0)

    def attend_row(i, carry):
        r = order(i)
        whole(sv, rv, r, a_send, a_recv).wait_recv()
        arrived = dot(perm[2], rv[r]).astype(BF16)
        qkv[...] = dot(arrived, wq[...]).astype(BF16)
        for here in columns:
            for four in quads:
                k = qkv[here, channels + four.start : channels + four.stop]
                scores[here, four] = dot_t(qkv[here, four], split_heads(k))
        for here in columns:
            for base in range(0, channels, 2 * head_dim):
                pair = slice(base, base + 2 * head_dim)
                s = scores[here, pair]
                peak_low = jnp.max(jnp.where(low, s, -jnp.inf), axis=-1, keepdims=True)
                peak_high = jnp.max(jnp.where(low, -jnp.inf, s), axis=-1, keepdims=True)
                peak = jnp.where(low, peak_low, peak_high)
                expo[here, pair] = jnp.exp2((s - peak) * log2e_scale).astype(BF16)
        for four in quads:
            for here in columns:
                v = qkv[here, 2 * channels + four.start : 2 * channels + four.stop]
                summed[here, four] = dot(expo[here, four], split_heads(v))
            total = dot(expo[:, four], ones[...])
            att[:, four] = (summed[:, four] / total).astype(BF16)
        av[r] = dot(perm[3], att[...]).astype(BF16)
        send_attended(r, i)
        return carry

    lax.fori_loop(0, rows, attend_row, 0)
    pass_whole().wait_recv()
    for k in range(2):
        from_relay(k).start()

    def out_row(i, carry):
        r = order(lax.rem(i + 1, rows))
        whole(av, ov, r, b_send, b_recv).wait_recv()
        attended = dot(perm[1], ov[r]).astype(BF16)
        total = mixed[r].astype(F32) + dot(attended, wo[...])
        out[:, r] = total.astype(BF16).reshape(frames, width, channels)
        return carry

    lax.fori_loop(0, rows, out_row, 0)

    pass_whole().wait_send()

    @pl.when(g > 0)
    def _():
        up.wait_send()

    @pl.when(g < ny - 1)
    def _():
        down.wait_send()

    for r in range(rows):

        @pl.when(t < n - 1)
        def _():
            hidden_copy(r).wait_send()

        whole(sv, rv, r, a_send, a_recv).wait_send()
        whole(av, ov, r, b_send, b_recv).wait_send()


def solution(mesh):
    n, ny = mesh.shape["ta"], mesh.shape["gy"]

    def per_device(clip, w_space, w_time, w_qkv, w_out, norm_gain):
        frames, rows, width, channels = clip.shape
        tokens = frames * width
        row_tokens = (rows, tokens, channels)
        dma = pltpu.SemaphoreType.DMA
        return pl.pallas_call(
            functools.partial(block_kernel, n, ny),
            out_shape=pltpu.VMEM(clip.shape, BF16),
            in_specs=[pl.BlockSpec(memory_space=pltpu.HBM)] * 6,
            out_specs=pl.BlockSpec(memory_space=pltpu.VMEM),
            scratch_shapes=[
                pltpu.VMEM((rows + 2, frames, width, channels), BF16),
                pltpu.VMEM((rows, frames + 2, width, channels), BF16),
                pltpu.VMEM(row_tokens, BF16),
                pltpu.VMEM(row_tokens, BF16),
                pltpu.VMEM(row_tokens, BF16),
                pltpu.VMEM(row_tokens, BF16),
                pltpu.VMEM(row_tokens, BF16),
                pltpu.VMEM((tokens, 3 * channels), BF16),
                pltpu.VMEM((tokens, channels), F32),
                pltpu.VMEM((tokens, channels), BF16),
                pltpu.VMEM((tokens, channels), F32),
                pltpu.VMEM((4 * n * frames, 4 * (channels // HEADS)), BF16),
                pltpu.VMEM((tokens, channels), BF16),
                pltpu.VMEM((4, tokens, tokens), BF16),
                pltpu.VMEM((3, 3 * channels, channels), BF16),
                pltpu.VMEM((3 * channels, channels), BF16),
                pltpu.VMEM((channels, 3 * channels), BF16),
                pltpu.VMEM((channels, channels), BF16),
                pltpu.VMEM((1, channels), F32),
                dma((rows,)),
                dma((3, 3)),
                dma((4,)),
                dma((2,)),
                dma((2,)),
                dma((rows,)),
                dma((rows,)),
                dma((rows,)),
                dma((rows,)),
                dma((rows,)),
                dma((rows,)),
                pltpu.SemaphoreType.REGULAR,
                pltpu.SemaphoreType.REGULAR,
                pltpu.SemaphoreType.REGULAR,
                pltpu.VMEM((2 * frames * (width // n), channels), BF16),
                dma,
                dma,
            ],
            compiler_params=pltpu.CompilerParams(
                collective_id=0, has_side_effects=True, vmem_limit_bytes=48 * 2**20
            ),
        )(
            *(
                pltpu.with_memory_space_constraint(a, pltpu.HBM)
                for a in (
                    clip,
                    w_space,
                    w_time.reshape(3 * channels, channels),
                    w_qkv,
                    w_out,
                    norm_gain.reshape(1, channels),
                )
            )
        )

    in_specs = (P(("ga", "ta"), "gy", None, None), P(), P(), P(), P(), P())
    out_specs = P(("ga", "ta"), "gy", None, None)
    return jax.shard_map(
        per_device, mesh=mesh, in_specs=in_specs, out_specs=out_specs, check_vma=False
    )
```

```python
import functools

import jax
import jax.numpy as jnp
from jax import lax
from jax.experimental import pallas as pl
from jax.experimental.pallas import tpu as pltpu
from jax.sharding import PartitionSpec as P

HEADS = 8
MESH = pl.DeviceIdType.MESH
F32 = jnp.float32
BF16 = jnp.bfloat16


def dot(a, b):
    return jnp.dot(a, b, preferred_element_type=F32)


def dot_t(a, b):
    return lax.dot_general(a, b, (((1,), (1,)), ((), ())), preferred_element_type=F32)


def block_kernel(
    n,
    ny,
    clip,
    w_space,
    w_time,
    w_qkv,
    w_out,
    gain,
    out,
    xv,
    hv,
    mixed,
    sv,
    rv,
    av,
    ov,
    qkv,
    scores,
    expo,
    summed,
    ones,
    att,
    perm,
    ws,
    wt,
    wq,
    wo,
    gv,
    clip_sem,
    ws_sem,
    w_sem,
    x_send,
    x_recv,
    h_send,
    h_recv,
    a_send,
    a_recv,
    b_send,
    b_recv,
    late,
    ready,
    next_ready,
    passing,
    pass_send,
    pass_recv,
):
    frames, rows, width, channels = clip.shape
    tokens = frames * width
    cols = width // n
    piece = frames * cols
    t = lax.axis_index("ta")
    g = lax.axis_index("gy")
    chips = n // 2
    chip, core = t // 2, lax.rem(t, 2)

    def peer(chip_off, core_off):
        return lax.rem(chip + chip_off + chips, chips) * 2 + lax.rem(core + core_off, 2)

    half = chips // 2
    early = 2 * (chips - 1 - half)
    offsets = [half]
    for d in range(half - 1, 0, -1):
        offsets += [d, -d]
    peers = [(c, k) for c in offsets for k in (0, 1)] + [(0, 1)]

    barrier = pltpu.get_barrier_semaphore()

    @pl.when(g > 0)
    def _():
        pl.semaphore_signal(barrier, inc=1, device_id={"gy": g - 1}, device_id_type=MESH)

    @pl.when(g < ny - 1)
    def _():
        pl.semaphore_signal(barrier, inc=1, device_id={"gy": g + 1}, device_id_type=MESH)

    @pl.when(t > 0)
    def _():
        for k in range(n):

            @pl.when((k > t) | (k == 0))
            def _():
                pl.semaphore_signal(barrier, inc=1, device_id={"ta": k}, device_id_type=MESH)

    beside = jnp.where(g < ny - 1, 1, 0) + jnp.where(g > 0, 1, 0)

    clip_loads = [
        pltpu.make_async_copy(clip.at[:, r], xv.at[r + 1], clip_sem.at[r]) for r in range(rows)
    ]
    for load in clip_loads:
        load.start()
    space_loads = []
    for b in range(3):
        for a in range(3):
            load = pltpu.make_async_copy(
                w_space.at[a, b], ws.at[b, pl.ds(a * channels, channels)], ws_sem.at[b, a]
            )
            load.start()
            space_loads.append(load)
    other_loads = [
        pltpu.make_async_copy(w_time, wt, w_sem.at[0]),
        pltpu.make_async_copy(w_qkv, wq, w_sem.at[1]),
        pltpu.make_async_copy(w_out, wo, w_sem.at[2]),
        pltpu.make_async_copy(gain, gv, w_sem.at[3]),
    ]

    up = pltpu.make_async_remote_copy(
        src_ref=clip.at[:, 0],
        dst_ref=xv.at[rows + 1],
        send_sem=x_send.at[0],
        recv_sem=x_recv.at[0],
        device_id={"gy": lax.rem(g + ny - 1, ny)},
        device_id_type=MESH,
    )
    down = pltpu.make_async_remote_copy(
        src_ref=clip.at[:, rows - 1],
        dst_ref=xv.at[0],
        send_sem=x_send.at[1],
        recv_sem=x_recv.at[1],
        device_id={"gy": lax.rem(g + 1, ny)},
        device_id_type=MESH,
    )
    pl.semaphore_wait(barrier, jnp.where(t == 0, n - 1, t - 1) + beside)

    @pl.when(g < ny - 1)
    def _():
        down.start()

    @pl.when(g > 0)
    def _():
        up.start()

    @pl.when(t > 1)
    def _():
        pl.semaphore_signal(next_ready, inc=1, device_id={"ta": t - 1}, device_id_type=MESH)

    for k in range(1, n):

        @pl.when(k < t)
        def _():
            pl.semaphore_signal(ready, inc=1, device_id={"ta": k}, device_id_type=MESH)

        @pl.when(t == 0)
        def _():
            pl.semaphore_signal(late, inc=1, device_id={"ta": k}, device_id_type=MESH)

    row_i = lax.broadcasted_iota(jnp.int32, (tokens, tokens), 0)
    col_i = lax.broadcasted_iota(jnp.int32, (tokens, tokens), 1)
    clip_len = n * frames
    natural = (
        lax.rem(row_i // cols, frames) * width + (row_i // piece) * cols + lax.rem(row_i, cols)
    )
    perm[0] = jnp.where(natural == col_i, 1.0, 0.0).astype(BF16)
    natural_t = (
        lax.rem(col_i // cols, frames) * width + (col_i // piece) * cols + lax.rem(col_i, cols)
    )
    perm[1] = jnp.where(natural_t == row_i, 1.0, 0.0).astype(BF16)
    by_col = lax.rem(row_i, clip_len) * cols + row_i // clip_len
    perm[2] = jnp.where(by_col == col_i, 1.0, 0.0).astype(BF16)
    by_col_t = lax.rem(col_i, clip_len) * cols + col_i // clip_len
    perm[3] = jnp.where(by_col_t == row_i, 1.0, 0.0).astype(BF16)

    @pl.when(g == 0)
    def _():
        xv[0] = jnp.zeros(xv.shape[1:], BF16)

    @pl.when(g == ny - 1)
    def _():
        xv[rows + 1] = jnp.zeros(xv.shape[1:], BF16)

    @pl.when(t == 0)
    def _():
        hv[:, 0:2] = jnp.zeros((rows, 2) + hv.shape[2:], BF16)

    def conv_frames(r, first, count, arrived=lambda b: None):
        these = count * width
        column = lax.rem(lax.broadcasted_iota(jnp.int32, (these, channels), 0), width)
        here = pl.ds(first, count)
        lhs = jnp.concatenate(
            [xv[r + a, here].reshape(these, channels) for a in range(3)], axis=1
        )
        arrived(0)
        left = pltpu.roll(dot(lhs, ws[0]), 1, 0)
        arrived(1)
        total = jnp.where(column == 0, 0.0, left) + dot(lhs, ws[1])
        arrived(2)
        right = pltpu.roll(dot(lhs, ws[2]), these - 1, 0)
        total = total + jnp.where(column == width - 1, 0.0, right)
        hidden = (total * jax.nn.sigmoid(total)).astype(BF16)
        hv[r, pl.ds(first + 2, count)] = hidden.reshape(count, width, channels)

    def hidden_copy(r):
        return pltpu.make_async_remote_copy(
            src_ref=hv.at[r, pl.ds(frames, 2)],
            dst_ref=hv.at[r, pl.ds(0, 2)],
            send_sem=h_send.at[r],
            recv_sem=h_recv.at[r],
            device_id={"ta": lax.rem(t + 1, n)},
            device_id_type=MESH,
        )

    def send_hidden(r):
        @pl.when(t < n - 1)
        def _():
            hidden_copy(r).start()

    def exchange(src, dst, r, dest, send_sem, recv_sem):
        return pltpu.make_async_remote_copy(
            src_ref=src.at[r, pl.ds(pl.multiple_of(dest * piece, piece), piece)],
            dst_ref=dst.at[r, pl.ds(pl.multiple_of(t * piece, piece), piece)],
            send_sem=send_sem.at[r],
            recv_sem=recv_sem.at[r],
            device_id={"ta": dest},
            device_id_type=MESH,
        )

    def keep_own(src, dst, r):
        own = pl.ds(pl.multiple_of(t * piece, piece), piece)
        dst[r, own] = src[r, own]

    def send_normed(r, i):
        for c, k in peers:
            dest = peer(c, k)

            @pl.when((dest > 0) | (i > 0))
            def _():
                exchange(sv, rv, r, dest, a_send, a_recv).start()

        keep_own(sv, rv, r)

    step = half // 2

    def to_relay(k):
        dest = peer(half, k)
        return pltpu.make_async_remote_copy(
            src_ref=av.at[1, pl.ds(pl.multiple_of(dest * piece, piece), piece)],
            dst_ref=passing.at[pl.ds(k * piece, piece)],
            send_sem=b_send.at[1],
            recv_sem=pass_recv,
            device_id={"ta": peer(-step, 0)},
            device_id_type=MESH,
        )

    def from_relay(k):
        origin = peer(step, 0)
        return pltpu.make_async_remote_copy(
            src_ref=passing.at[pl.ds(k * piece, piece)],
            dst_ref=ov.at[1, pl.ds(pl.multiple_of(origin * piece, piece), piece)],
            send_sem=pass_send,
            recv_sem=b_recv.at[1],
            device_id={"ta": peer(-step, k)},
            device_id_type=MESH,
        )

    def pass_whole():
        return pltpu.make_async_remote_copy(
            src_ref=passing,
            dst_ref=passing,
            send_sem=pass_send,
            recv_sem=pass_recv,
            device_id={"ta": peer(-step, 0)},
            device_id_type=MESH,
        )

    def send_attended(r, i):
        for c, k in peers:
            if c == half:

                @pl.when(i == 0)
                def _():
                    to_relay(k).start()

                @pl.when(i > 0)
                def _():
                    exchange(av, ov, r, peer(c, k), b_send, b_recv).start()

            else:
                exchange(av, ov, r, peer(c, k), b_send, b_recv).start()
        keep_own(av, ov, r)

    def whole(src, dst, r, send_sem, recv_sem):
        return pltpu.make_async_remote_copy(
            src_ref=src.at[r, pl.ds(0, (n - 1) * piece)],
            dst_ref=dst.at[r, pl.ds(0, (n - 1) * piece)],
            send_sem=send_sem.at[r],
            recv_sem=recv_sem.at[r],
            device_id={"ta": lax.rem(t + 1, n)},
            device_id_type=MESH,
        )

    def temporal_row(r):
        @pl.when(t > 0)
        def _():
            hidden_copy(r).wait_recv()

        lhs = jnp.concatenate(
            [hv[r, 2 - k : 2 - k + frames].reshape(tokens, channels) for k in range(3)], axis=1
        )
        total = xv[r + 1].reshape(tokens, channels).astype(F32) + dot(lhs, wt[...])
        rounded = total.astype(BF16)
        mixed[r] = rounded
        wide = rounded.astype(F32)
        scale = lax.rsqrt(jnp.mean(wide * wide, axis=-1, keepdims=True) + 1e-06)
        normed = (wide * scale * gv[...]).astype(BF16)
        sv[r] = dot(perm[0], normed).astype(BF16)

    def space_arrived(b):
        for load in space_loads[3 * b : 3 * b + 3]:
            load.wait()

    for load in clip_loads:
        load.wait()
    conv_frames(1, frames - 2, 2, space_arrived)
    for load in other_loads:
        load.start()

    @pl.when((t > 0) & (t < n - 1))
    def _():
        pl.semaphore_wait(next_ready, 1)

    send_hidden(1)

    def inner_last(r, c):
        conv_frames(r, frames - 2, 2)
        send_hidden(r)
        return c

    def inner_first(r, c):
        conv_frames(r, 0, frames - 2)
        return c

    lax.fori_loop(2, rows - 1, inner_last, 0)
    lax.fori_loop(1, rows - 1, inner_first, 0)
    for load in other_loads:
        load.wait()

    def order(i):
        return jnp.where(i < rows - 2, i + 1, (i - (rows - 2)) * (rows - 1))

    def temporal(i, c):
        r = order(i)
        temporal_row(r)

        @pl.when((i == 0) & (t > 0) & (t < n - 1))
        def _():
            pl.semaphore_wait(ready, n - 1 - t)

        @pl.when((i == 1) & (t > 0))
        def _():
            pl.semaphore_wait(late, 1)
            exchange(sv, rv, order(0), 0, a_send, a_recv).start()

        send_normed(r, i)
        return c

    before = jnp.where((t == 0) | (t >= early), 1, 0)
    lax.fori_loop(0, before, temporal, 0)

    @pl.when(g > 0)
    def _():
        down.wait_recv()

    @pl.when(g < ny - 1)
    def _():
        up.wait_recv()

    def edge(i, c):
        r = i * (rows - 1)
        conv_frames(r, 0, frames)
        send_hidden(r)
        return c

    lax.fori_loop(0, 2, edge, 0)
    lax.fori_loop(before, rows, temporal, 0)

    head_dim = channels // HEADS
    quad = 4 * head_dim
    low = lax.broadcasted_iota(jnp.int32, (clip_len, 2 * head_dim), 1) < head_dim
    head_of = lax.broadcasted_iota(jnp.int32, (clip_len, quad), 1) // head_dim
    ones_row = lax.broadcasted_iota(jnp.int32, (4 * clip_len, quad), 0) // clip_len
    ones_col = lax.broadcasted_iota(jnp.int32, (4 * clip_len, quad), 1) // head_dim
    ones[...] = jnp.where(ones_row == ones_col, 1.0, 0.0).astype(BF16)
    log2e_scale = 1.4426950408889634 / head_dim**0.5
    columns = [slice(c * clip_len, (c + 1) * clip_len) for c in range(cols)]
    quads = [slice(base, base + quad) for base in range(0, channels, quad)]

    def split_heads(x):
        zero = jnp.zeros_like(x)
        return jnp.concatenate([jnp.where(head_of == h, x, zero) for h in range(4)], axis=0)

    def attend_row(i, carry):
        r = order(i)
        whole(sv, rv, r, a_send, a_recv).wait_recv()
        arrived = dot(perm[2], rv[r]).astype(BF16)
        qkv[...] = dot(arrived, wq[...]).astype(BF16)
        for here in columns:
            for four in quads:
                k = qkv[here, channels + four.start : channels + four.stop]
                scores[here, four] = dot_t(qkv[here, four], split_heads(k))
        for here in columns:
            for base in range(0, channels, 2 * head_dim):
                pair = slice(base, base + 2 * head_dim)
                s = scores[here, pair]
                peak_low = jnp.max(jnp.where(low, s, -jnp.inf), axis=-1, keepdims=True)
                peak_high = jnp.max(jnp.where(low, -jnp.inf, s), axis=-1, keepdims=True)
                peak = jnp.where(low, peak_low, peak_high)
                expo[here, pair] = jnp.exp2((s - peak) * log2e_scale).astype(BF16)
        for four in quads:
            for here in columns:
                v = qkv[here, 2 * channels + four.start : 2 * channels + four.stop]
                summed[here, four] = dot(expo[here, four], split_heads(v))
            total = dot(expo[:, four], ones[...])
            att[:, four] = (summed[:, four] / total).astype(BF16)
        av[r] = dot(perm[3], att[...]).astype(BF16)
        @pl.when(i == rows - 1)
        def _():
            pass_whole().wait_recv()
            for k in range(2):
                from_relay(k).start()

        send_attended(r, i)
        return carry

    lax.fori_loop(0, rows, attend_row, 0)

    def out_row(i, carry):
        r = order(jnp.where(i < rows - 1, lax.rem(i + 1, rows - 1), rows - 1))
        whole(av, ov, r, b_send, b_recv).wait_recv()
        attended = dot(perm[1], ov[r]).astype(BF16)
        total = mixed[r].astype(F32) + dot(attended, wo[...])
        out[:, r] = total.astype(BF16).reshape(frames, width, channels)
        return carry

    lax.fori_loop(0, rows, out_row, 0)

    pass_whole().wait_send()

    @pl.when(g > 0)
    def _():
        up.wait_send()

    @pl.when(g < ny - 1)
    def _():
        down.wait_send()

    for r in range(rows):

        @pl.when(t < n - 1)
        def _():
            hidden_copy(r).wait_send()

        whole(sv, rv, r, a_send, a_recv).wait_send()
        whole(av, ov, r, b_send, b_recv).wait_send()


def solution(mesh):
    n, ny = mesh.shape["ta"], mesh.shape["gy"]

    def per_device(clip, w_space, w_time, w_qkv, w_out, norm_gain):
        frames, rows, width, channels = clip.shape
        tokens = frames * width
        row_tokens = (rows, tokens, channels)
        dma = pltpu.SemaphoreType.DMA
        return pl.pallas_call(
            functools.partial(block_kernel, n, ny),
            out_shape=pltpu.VMEM(clip.shape, BF16),
            in_specs=[pl.BlockSpec(memory_space=pltpu.HBM)] * 6,
            out_specs=pl.BlockSpec(memory_space=pltpu.VMEM),
            scratch_shapes=[
                pltpu.VMEM((rows + 2, frames, width, channels), BF16),
                pltpu.VMEM((rows, frames + 2, width, channels), BF16),
                pltpu.VMEM(row_tokens, BF16),
                pltpu.VMEM(row_tokens, BF16),
                pltpu.VMEM(row_tokens, BF16),
                pltpu.VMEM(row_tokens, BF16),
                pltpu.VMEM(row_tokens, BF16),
                pltpu.VMEM((tokens, 3 * channels), BF16),
                pltpu.VMEM((tokens, channels), F32),
                pltpu.VMEM((tokens, channels), BF16),
                pltpu.VMEM((tokens, channels), F32),
                pltpu.VMEM((4 * n * frames, 4 * (channels // HEADS)), BF16),
                pltpu.VMEM((tokens, channels), BF16),
                pltpu.VMEM((4, tokens, tokens), BF16),
                pltpu.VMEM((3, 3 * channels, channels), BF16),
                pltpu.VMEM((3 * channels, channels), BF16),
                pltpu.VMEM((channels, 3 * channels), BF16),
                pltpu.VMEM((channels, channels), BF16),
                pltpu.VMEM((1, channels), F32),
                dma((rows,)),
                dma((3, 3)),
                dma((4,)),
                dma((2,)),
                dma((2,)),
                dma((rows,)),
                dma((rows,)),
                dma((rows,)),
                dma((rows,)),
                dma((rows,)),
                dma((rows,)),
                pltpu.SemaphoreType.REGULAR,
                pltpu.SemaphoreType.REGULAR,
                pltpu.SemaphoreType.REGULAR,
                pltpu.VMEM((2 * frames * (width // n), channels), BF16),
                dma,
                dma,
            ],
            compiler_params=pltpu.CompilerParams(
                collective_id=0, has_side_effects=True, vmem_limit_bytes=48 * 2**20
            ),
        )(
            *(
                pltpu.with_memory_space_constraint(a, pltpu.HBM)
                for a in (
                    clip,
                    w_space,
                    w_time.reshape(3 * channels, channels),
                    w_qkv,
                    w_out,
                    norm_gain.reshape(1, channels),
                )
            )
        )

    in_specs = (P(("ga", "ta"), "gy", None, None), P(), P(), P(), P(), P())
    out_specs = P(("ga", "ta"), "gy", None, None)
    return jax.shard_map(
        per_device, mesh=mesh, in_specs=in_specs, out_specs=out_specs, check_vma=False
    )
```
